256 devices in a mesh: seq: 128 (over z, x, y), tp: 2 (over core).
Axes of the slice: x: 4, y: 4, z: 8, core: 2. Of those that a mesh axis runs over, the one named last changes fastest.
Arguments:
- img_qkv: bfloat16 [1, 4096, 3, 2048], P(None, 'seq', None, 'tp'), may hold values from -7 to 7
- txt_qkv: bfloat16 [1, 256, 3, 2048], P(None, None, None, 'tp'), may hold values from -7 to 7
- frame_index: int32 [1, 4096], P(None, 'seq'), may hold values from 0 to 32
- row_index: int32 [1, 4096], P(None, 'seq'), may hold values from 0 to 44
- column_index: int32 [1, 4096], P(None, 'seq'), may hold values from 0 to 79
- txt_len: int32 [1], replicated, may hold values from 64 to 256
- residual: bfloat16 [1, 4096, 3072], P(None, ('seq', 'tp')), may hold values from -6 to 6
- w_proj: bfloat16 [2048, 3072], P('tp'), may hold values from -0.125 to 0.125
- proj_bias: float32 [3072], replicated, may hold values from -3 to 3
- gate: float32 [3072], replicated, may hold values from -4 to 4
Outputs:
- img_out: bfloat16 [1, 4096, 3072], P(None, ('seq', 'tp'))
- txt_out: bfloat16 [1, 256, 2048], P(None, None, 'tp')
The draws below stay inside these ranges and needn't reach their ends.
All inputs are finite; a program needn't handle non-finite values.
Results may differ from the reference program's by a relative error of at most 0.0082.
Values may be sent and summed in bfloat16 or wider, within the bound.
A program may use at most 64 MiB of HBM per device.

```python
import math
import jax
import jax.numpy as jnp
from jax import lax

D = 3072
HD = 128
HEADS = 16
TXT = 256
LAT_T = 33
LAT_H = 45
LAT_W = 80
CLIPS = 1
IMG = 4096
QW = 2048


def draw_img_qkv(key, part):
    width_all = HEADS * HD
    total_rows = CLIPS * IMG
    subkeys = jax.random.split(jax.random.fold_in(key, 11), 4)
    query_part = jnp.clip(1.8 * jax.random.normal(subkeys[0], (total_rows, width_all), jnp.float32), -7.0, 7.0)
    key_part = jnp.clip(1.8 * jax.random.normal(subkeys[1], (total_rows, width_all), jnp.float32), -7.0, 7.0)
    value_part = jnp.clip(jax.random.normal(subkeys[3], (total_rows, width_all), jnp.float32), -6.0, 6.0)
    stacked = jnp.stack([query_part, key_part, value_part], axis=1)
    return stacked.reshape(CLIPS, IMG, 3, width_all).astype(jnp.bfloat16)


def draw_txt_qkv(key, part):
    width_all = HEADS * HD
    subkeys = jax.random.split(jax.random.fold_in(key, 23), 4)
    query_part = jnp.clip(1.8 * jax.random.normal(subkeys[0], (CLIPS, TXT, width_all), jnp.float32), -7.0, 7.0)
    key_part = jnp.clip(1.8 * jax.random.normal(subkeys[1], (CLIPS, TXT, width_all), jnp.float32), -7.0, 7.0)
    value_part = jnp.clip(jax.random.normal(subkeys[3], (CLIPS, TXT, width_all), jnp.float32), -6.0, 6.0)
    return jnp.stack([query_part, key_part, value_part], axis=2).astype(jnp.bfloat16)


def plant(values, own_key, low, high):
    extent = values.shape
    index_at = [jax.random.randint(jax.random.fold_in(own_key, axis), (), 0, extent[axis]) for axis in range(len(extent))]
    values = values.at[tuple(index_at)].set(low)
    longest = extent.index(max(extent))
    index_at[longest] = (index_at[longest] + 1) % extent[longest]
    return values.at[tuple(index_at)].set(high)


def steps_of(key, dims, cuts, least, high):
    def one(dim, parts):
        steps = jax.random.uniform(jax.random.fold_in(jax.random.fold_in(key, 6), dim), (parts,), jnp.float32, least / len(cuts), high / len(cuts))
        return jnp.repeat(jnp.exp(steps), dims[dim] // parts).reshape((-1,) + (1,) * (len(dims) - dim - 1))

    factor_of = one(*cuts[0])
    for cut in cuts[1:]:
        factor_of = factor_of * one(*cut)
    return factor_of


def normal_values(rng, shape, scale, limit, cuts=(), held_as=jnp.bfloat16):
    values = scale * jax.random.normal(rng, shape, jnp.float32)
    if cuts:
        values = values * steps_of(rng, shape, cuts, -0.22, 0.18)
    return jnp.clip(values, -limit, limit).astype(held_as)


def setup_inputs(seed: int = 0) -> dict:
    seeds = jax.random.split(jax.random.key(seed), 11)
    img_qkv = draw_img_qkv(jax.random.fold_in(seeds[10], 71), 0)
    txt_qkv = draw_txt_qkv(jax.random.fold_in(seeds[10], 71), 0)
    frame_index = plant(jax.random.randint(seeds[2], (CLIPS, IMG), 0, LAT_T), jax.random.fold_in(seeds[2], 1), 0, LAT_T - 1).astype(jnp.int32)
    row_index = plant(jax.random.randint(seeds[3], (CLIPS, IMG), 0, LAT_H), jax.random.fold_in(seeds[3], 1), 0, LAT_H - 1).astype(jnp.int32)
    column_index = plant(jax.random.randint(seeds[4], (CLIPS, IMG), 0, LAT_W), jax.random.fold_in(seeds[4], 1), 0, LAT_W - 1).astype(jnp.int32)
    txt_len = jax.random.randint(seeds[5], (CLIPS,), TXT // 4, TXT + 1).astype(jnp.int32)
    residual = normal_values(seeds[6], (CLIPS, IMG, D), 1.0, 6.0, ((1, 256),))
    w_proj = normal_values(seeds[7], (QW, D), QW ** -0.5, 0.125, ((0, 2),))
    proj_bias = normal_values(seeds[8], (D,), 0.5, 3.0, (), jnp.float32)
    gate = normal_values(seeds[9], (D,), 1.0, 4.0, (), jnp.float32)
    return {"img_qkv": img_qkv, "txt_qkv": txt_qkv, "frame_index": frame_index, "row_index": row_index, "column_index": column_index, "txt_len": txt_len, "residual": residual, "w_proj": w_proj, "proj_bias": proj_bias, "gate": gate}


rope_base = 256.0
neg_large = -1e+30

def rope_tables(frame_index, row_index, column_index, head_dim):
    frame_part = head_dim // 8
    second = (head_dim - frame_part) // 2
    pieces = []
    for places, part_width in ((frame_index, frame_part), (row_index, second), (column_index, second)):
        pair_ids = jnp.arange(part_width // 2).astype(jnp.float32)
        pair_rates = rope_base ** (-2.0 * pair_ids / part_width)
        pieces.append(places.astype(jnp.float32)[:, None] * pair_rates[None, :])
    angles = jnp.repeat(jnp.concatenate(pieces, axis=1), 2, axis=1)
    parity = jnp.arange(head_dim) % 2
    signed = jnp.where(parity == 0, -1.0, 1.0).astype(jnp.float32)
    return (jnp.cos(angles), jnp.sin(angles) * signed[None, :])

def rotate(block_in, cosine, sine_table):
    values = block_in.astype(jnp.float32)
    parity = jnp.arange(values.shape[-1]) % 2
    partner = jnp.where(parity == 0, jnp.roll(values, -1, axis=-1), jnp.roll(values, 1, axis=-1))
    return (values * cosine[:, None, :] + partner * sine_table[:, None, :]).astype(jnp.bfloat16)

def attend_head(query_head, key_head, value_head, live_keys):
    row_count = query_head.shape[0]
    row_block = 1
    for candidate in range(1, 1025):
        if row_count % candidate == 0:
            row_block = candidate
    blocks = query_head.reshape(row_count // row_block, row_block, query_head.shape[1])
    score_scale = 1.0 / math.sqrt(query_head.shape[1])

    def one_block(query_block):
        scores = jnp.dot(query_block, key_head.T, preferred_element_type=jnp.float32) * score_scale
        scores = jnp.where(live_keys[None, :], scores, neg_large)
        peak = lax.optimization_barrier(jnp.max(scores, axis=1, keepdims=True))
        weights = jnp.where(live_keys[None, :], jnp.exp(scores - peak), 0.0)
        weight_sum = lax.optimization_barrier(jnp.sum(weights, axis=1, keepdims=True))
        blended = jnp.dot(weights.astype(jnp.bfloat16), value_head, preferred_element_type=jnp.float32)
        return (blended / weight_sum).astype(jnp.bfloat16)
    return lax.map(one_block, blocks).reshape(row_count, query_head.shape[1])

def clip_attention(clip_qkv, clip_txt, frames, rows_at, columns_at, length):
    cosine, sine_table = rope_tables(frames, rows_at, columns_at, HD)
    img_query = rotate(clip_qkv[:, 0].reshape(IMG, HEADS, HD), cosine, sine_table)
    img_key = rotate(clip_qkv[:, 1].reshape(IMG, HEADS, HD), cosine, sine_table)
    img_value = clip_qkv[:, 2].reshape(IMG, HEADS, HD)
    queries = jnp.concatenate([img_query, clip_txt[:, 0].reshape(TXT, HEADS, HD)], axis=0)
    all_keys = jnp.concatenate([img_key, clip_txt[:, 1].reshape(TXT, HEADS, HD)], axis=0)
    all_values = jnp.concatenate([img_value, clip_txt[:, 2].reshape(TXT, HEADS, HD)], axis=0)
    live_keys = jnp.arange(IMG + TXT) < IMG + length

    def head_work(operands):
        return attend_head(operands[0], operands[1], operands[2], live_keys)
    attended = lax.map(head_work, (queries.transpose(1, 0, 2), all_keys.transpose(1, 0, 2), all_values.transpose(1, 0, 2)))
    joined = attended.transpose(1, 0, 2).reshape(IMG + TXT, HEADS * HD)
    img_rows = joined[:IMG]
    txt_rows = joined[IMG:]
    txt_live = jnp.arange(TXT) < length
    txt_rows = jnp.where(txt_live[:, None], txt_rows, jnp.zeros_like(txt_rows))
    return (img_rows, txt_rows)

def reference(img_qkv, txt_qkv, frame_index, row_index, column_index, txt_len, residual, w_proj, proj_bias, gate):
    img_outs = []
    txt_outs = []
    for clip in range(CLIPS):
        img_rows, txt_rows = clip_attention(img_qkv[clip], txt_qkv[clip], frame_index[clip], row_index[clip], column_index[clip], txt_len[clip])
        projected = jnp.dot(img_rows, w_proj, preferred_element_type=jnp.float32)
        mixed = residual[clip].astype(jnp.float32) + gate[None, :] * (projected + proj_bias[None, :])
        img_outs.append(mixed.astype(jnp.bfloat16))
        txt_outs.append(txt_rows)
    return (jnp.stack(img_outs, axis=0), jnp.stack(txt_outs, axis=0))
```

```python
import math

import jax
import jax.numpy as jnp
from jax import lax
from jax.experimental import pallas as pl
from jax.experimental.pallas import tpu as pltpu
from jax.sharding import Mesh
from jax.sharding import PartitionSpec as P

HD = 128
AX_Z, AX_X, AX_Y, AX_C = "seq_0", "seq_1", "seq_2", "tp"
SEQ = (AX_Z, AX_X, AX_Y)
SEQ_TP = (AX_Z, AX_X, AX_Y, AX_C)
MESH = pl.DeviceIdType.MESH
F32 = jnp.float32
BF16 = jnp.bfloat16

rope_base = 256.0
neg_large = -1e30


def rope_in_kernel(frames, rows, columns, tok):
    part0 = HD // 8
    part1 = (HD - part0) // 2
    eye = lax.broadcasted_iota(jnp.int32, (tok, tok), 0) == lax.broadcasted_iota(jnp.int32, (tok, tok), 1)

    def column(ref):
        places = jnp.broadcast_to(ref[...].astype(F32), (tok, tok))
        return jnp.sum(jnp.where(eye, places, 0.0), axis=1, keepdims=True)

    lane = lax.broadcasted_iota(jnp.int32, (tok, HD), 1)
    in0 = lane < part0
    in1 = lane < part0 + part1
    start = jnp.where(in0, 0, jnp.where(in1, part0, part0 + part1))
    pair = ((lane - start) >> 1).astype(F32)
    width = jnp.where(in0, float(part0), float(part1))
    rate = jnp.exp(pair * (-2.0 * math.log(rope_base)) / width)
    place = jnp.where(in0, column(frames), jnp.where(in1, column(rows), column(columns)))
    angle = place * rate
    cosine, sine = jnp.cos(angle), jnp.sin(angle)
    even = (lane & 1) == 0
    return cosine, jnp.where(even, -sine, 0.0), jnp.where(even, 0.0, sine)


def kernel_body(
    Z, X, Y, tok,
    qkv_hbm, txt_hbm, w_hbm, frames, rows, columns, txt_len,
    p_out, t_out,
    qkv_v, w_v, tq, tk, tv, send, qg, kvg, ob, st, orecv, srecv, tob, tst, torecv, tsrecv,
    zs, ar, tbuf, part_own, part_send, part_recv,
    local_sem, zq_sem, zkv_sem, z_send, xq_sem, xq_send, ykv_sem, ykv_send,
    xo_sem, xs_sem, xo_send, xs_send, xto_sem, xts_sem, xto_send, xts_send,
    zo_sem, zo_send, t2_sem, t2_send, t3_sem, t3_send, c_sem, c_send,
):
    z, x, y, c = (lax.axis_index(a) for a in SEQ_TP)
    txt_q = tq.shape[0]
    txt_k = tk.shape[0]
    scale2 = math.log2(math.e) / math.sqrt(HD)

    def put(src, dst, ssem, rsem, axis, to):
        pltpu.make_async_remote_copy(
            src_ref=src, dst_ref=dst, send_sem=ssem, recv_sem=rsem,
            device_id={axis: to}, device_id_type=MESH,
        ).start()

    def await_bytes(ref, sem):
        pltpu.make_async_copy(ref, ref, sem).wait()

    barrier = pltpu.get_barrier_semaphore()
    peers = 0
    for axis, size, me in ((AX_Z, Z, z), (AX_X, X, x), (AX_Y, Y, y), (AX_C, 2, c)):
        for step in range(1, size):
            pl.semaphore_signal(barrier, inc=1, device_id={axis: lax.rem(me + step, size)}, device_id_type=MESH)
            peers += 1

    lane0 = pl.multiple_of(z * HD, HD)
    get_qkv = pltpu.make_async_copy(qkv_hbm, qkv_v, local_sem.at[0])
    get_qkv.start()
    get_tq = pltpu.make_async_copy(
        txt_hbm.at[0, pl.ds(pl.multiple_of(y * txt_q, txt_q), txt_q), pl.ds(lane0, HD)], tq, local_sem.at[1])
    get_tk = pltpu.make_async_copy(
        txt_hbm.at[1, pl.ds(pl.multiple_of(x * txt_k, txt_k), txt_k), pl.ds(lane0, HD)], tk, local_sem.at[2])
    get_tv = pltpu.make_async_copy(
        txt_hbm.at[2, pl.ds(pl.multiple_of(x * txt_k, txt_k), txt_k), pl.ds(lane0, HD)], tv, local_sem.at[3])
    get_w = pltpu.make_async_copy(w_hbm, w_v, local_sem.at[4])
    for get in (get_tq, get_tk, get_tv, get_w):
        get.start()

    cosine, sine_even, sine_odd = rope_in_kernel(frames, rows, columns, tok)
    get_qkv.wait()
    for h in range(Z):
        lanes = slice(h * HD, (h + 1) * HD)
        for kind in range(2):
            block = qkv_v[kind, :, lanes].astype(F32)
            turned = (
                block * cosine
                + pltpu.roll(block, HD - 1, 1) * sine_even
                + pltpu.roll(block, 1, 1) * sine_odd
            )
            send[h, kind] = turned.astype(BF16)
        send[h, 2] = qkv_v[2, :, lanes]
    qg[x, z] = send[z, 0]
    kvg[y, z] = send[z, 1:3]

    pl.semaphore_wait(barrier, peers)

    order = sorted(range(1, Z), key=lambda step: -min(step, Z - step))
    for step in order:
        to = lax.rem(z + step, Z)
        put(send.at[to, 1:3], kvg.at[y, z], z_send, zkv_sem.at[z], AX_Z, to)
        put(send.at[to, 0], qg.at[x, z], z_send, zq_sem.at[z], AX_Z, to)

    for step in [0] + order:
        source = lax.rem(z + step, Z)
        if step:
            await_bytes(kvg.at[y, source], zkv_sem.at[source])
        for hop in range(1, Y):
            put(kvg.at[y, source], kvg.at[y, source], ykv_send, ykv_sem.at[y], AX_Y, lax.rem(y + hop, Y))
        if step:
            await_bytes(qg.at[x, source], zq_sem.at[source])
        for hop in range(1, X):
            put(qg.at[x, source], qg.at[x, source], xq_send, xq_sem.at[x], AX_X, lax.rem(x + hop, X))

    for get in (get_tq, get_tk, get_tv):
        get.wait()
    for hop in range(1, Y):
        other = lax.rem(y + hop, Y)
        await_bytes(kvg.at[other], ykv_sem.at[other])
    for hop in range(1, X):
        other = lax.rem(x + hop, X)
        await_bytes(qg.at[other], xq_sem.at[other])

    keys_n = Y * Z * tok
    live = lax.broadcasted_iota(jnp.int32, (1, txt_k), 1) < txt_len[0] - x * txt_k

    def scores_of(queries, keys):
        return lax.dot_general(queries, keys, (((1,), (1,)), ((), ())), preferred_element_type=F32)

    def attend(queries):
        scores = scores_of(queries, kvg[:, :, 0].reshape(keys_n, HD))
        txt_scores = jnp.where(live, scores_of(queries, tk[...]), neg_large)
        peak = jnp.maximum(
            jnp.max(scores, axis=1, keepdims=True), jnp.max(txt_scores, axis=1, keepdims=True))
        weights = jnp.exp2((scores - peak) * scale2)
        txt_weights = jnp.exp2((txt_scores - peak) * scale2)
        total = jnp.sum(weights, axis=1, keepdims=True) + jnp.sum(txt_weights, axis=1, keepdims=True)
        blended = jnp.dot(
            weights.astype(BF16), kvg[:, :, 1].reshape(keys_n, HD), preferred_element_type=F32)
        blended += jnp.dot(txt_weights.astype(BF16), tv[...], preferred_element_type=F32)
        return blended / total, peak * scale2 + jnp.log2(total)

    def to_row(col):
        n = col.shape[0]
        eye = lax.broadcasted_iota(jnp.int32, (n, HD), 0) == lax.broadcasted_iota(jnp.int32, (n, HD), 1)
        return jnp.sum(jnp.where(eye, jnp.broadcast_to(col, (n, HD)), 0.0), axis=0, keepdims=True)

    def to_col(row, n):
        eye = lax.broadcasted_iota(jnp.int32, (n, HD), 0) == lax.broadcasted_iota(jnp.int32, (n, HD), 1)
        return jnp.sum(jnp.where(eye, jnp.broadcast_to(row, (n, HD)), 0.0), axis=1, keepdims=True)

    def merge(values, logs):
        top = logs[0]
        for log in logs[1:]:
            top = jnp.maximum(top, log)
        shares = [jnp.exp2(log - top) for log in logs]
        return sum(v * s for v, s in zip(values, shares)) / sum(shares)

    part, log = attend(tq[...])
    tob[...] = part.astype(BF16)
    tst[...] = to_row(log)
    for hop in range(1, X):
        to = lax.rem(x + hop, X)
        put(tob, torecv.at[x], xto_send.at[hop], xto_sem.at[x], AX_X, to)
        put(tst, tsrecv.at[x], xts_send.at[hop], xts_sem.at[x], AX_X, to)

    block_n = Z * tok
    strips = block_n // HD
    for hop in sorted(range(1, X), key=lambda hop: -min(hop, X - hop)) + [0]:
        to = lax.rem(x + hop, X)
        part, log = attend(qg[to].reshape(block_n, HD))
        ob[to] = part.astype(BF16)
        for strip in range(strips):
            st[to, strip] = to_row(log[strip * HD:(strip + 1) * HD])
        if hop:
            put(ob.at[to], orecv.at[x], xo_send.at[hop], xo_sem.at[x], AX_X, to)
            put(st.at[to], srecv.at[x], xs_send.at[hop], xs_sem.at[x], AX_X, to)

    values, logs = [tob[...].astype(F32)], [to_col(tst[...], txt_q)]
    for hop in range(1, X):
        other = lax.rem(x + hop, X)
        await_bytes(torecv.at[other], xto_sem.at[other])
        await_bytes(tsrecv.at[other], xts_sem.at[other])
        values.append(torecv[other].astype(F32))
        logs.append(to_col(tsrecv[other], txt_q))
    kept = lax.broadcasted_iota(jnp.int32, (txt_q, 1), 0) + y * txt_q < txt_len[0]
    tbuf[y, z] = jnp.where(kept, merge(values, logs), 0.0).astype(BF16)

    values, logs = [ob[x].astype(F32)], [[to_col(st[x, strip], HD) for strip in range(strips)]]
    for hop in range(1, X):
        other = lax.rem(x + hop, X)
        await_bytes(orecv.at[other], xo_sem.at[other])
        await_bytes(srecv.at[other], xs_sem.at[other])
        values.append(orecv[other].astype(F32))
        logs.append([to_col(srecv[other, strip], HD) for strip in range(strips)])
    for strip in range(strips):
        rows_at = slice(strip * HD, (strip + 1) * HD)
        mixed = merge([v[rows_at] for v in values], [g[strip] for g in logs]).astype(BF16)
        per = HD // tok
        zs[strip * per:(strip + 1) * per] = mixed.reshape(per, tok, HD)
    ar[z] = zs[z]
    for step in order:
        to = lax.rem(z + step, Z)
        put(zs.at[to], ar.at[z], zo_send, zo_sem, AX_Z, to)
    for step in order:
        to = lax.rem(z + step, Z)
        put(tbuf.at[y, z], tbuf.at[y, z], t2_send, t2_sem, AX_Z, to)

    await_bytes(ar.at[0:Z - 1], zo_sem)
    get_w.wait()
    mine = jnp.concatenate([ar[h] for h in range(Z)], axis=1)
    half = tok // 2
    cuts = part_send.shape[0]
    wide = part_send.shape[2]
    for cut in range(cuts):
        lanes = slice(cut * wide, (cut + 1) * wide)
        product = jnp.dot(mine, w_v[:, lanes], preferred_element_type=F32)
        upper, lower = product[:half], product[half:]
        part_own[:, lanes] = jnp.where(c == 0, upper, lower)
        part_send[cut] = jnp.where(c == 0, lower, upper).astype(BF16)
        put(part_send.at[cut], part_recv.at[cut], c_send.at[cut], c_sem.at[cut], AX_C, 1 - c)

    await_bytes(tbuf.at[0, 0:Z - 1], t2_sem)
    for hop in range(1, Y):
        put(tbuf.at[y], tbuf.at[y], t3_send, t3_sem.at[y], AX_Y, lax.rem(y + hop, Y))
    out_copies = [pltpu.make_async_copy(tbuf.at[y], t_out.at[y], local_sem.at[5])]
    out_copies[0].start()

    for cut in range(cuts):
        lanes = slice(cut * wide, (cut + 1) * wide)
        await_bytes(part_recv.at[cut], c_sem.at[cut])
        p_out[:, lanes] = part_own[:, lanes] + part_recv[cut].astype(F32)

    for hop in range(1, Y):
        other = lax.rem(y + hop, Y)
        await_bytes(tbuf.at[other], t3_sem.at[other])
        out = pltpu.make_async_copy(tbuf.at[other], t_out.at[other], local_sem.at[5 + hop])
        out.start()
        out_copies.append(out)

    await_bytes(send.at[0:Z - 1], z_send)
    await_bytes(kvg.at[0:Y - 1], ykv_send)
    await_bytes(qg.at[0:X - 1], xq_send)
    for hop in range(1, X):
        await_bytes(tob, xto_send.at[hop])
        await_bytes(tst, xts_send.at[hop])
        await_bytes(ob.at[0], xo_send.at[hop])
        await_bytes(st.at[0], xs_send.at[hop])
    await_bytes(zs.at[0:Z - 1], zo_send)
    await_bytes(tbuf.at[0, 0:Z - 1], t2_send)
    await_bytes(tbuf.at[0:Y - 1], t3_send)
    for cut in range(cuts):
        await_bytes(part_send.at[cut], c_send.at[cut])
    for out in out_copies:
        out.wait()


def shards(
    img_qkv, txt_qkv, frame_index, row_index, column_index, txt_len, residual, w_proj, proj_bias, gate,
):
    Z, X, Y = (lax.axis_size(a) for a in SEQ)
    tok = img_qkv.shape[1]
    width = img_qkv.shape[3]
    txt_total = txt_qkv.shape[1]
    out_width = w_proj.shape[1]
    txt_q, txt_k = txt_total // Y, txt_total // X
    cuts = 6
    wide = out_width // cuts
    half = tok // 2
    block_n = Z * tok
    strips = block_n // HD

    qkv = jnp.transpose(img_qkv[0], (1, 0, 2))
    txt = jnp.transpose(txt_qkv[0], (1, 0, 2))
    dma = pltpu.SemaphoreType.DMA
    vm = pltpu.VMEM
    any_spec = pl.BlockSpec(memory_space=pltpu.HBM)
    vmem_spec = pl.BlockSpec(memory_space=pltpu.VMEM)

    def body(*refs):
        kernel_body(Z, X, Y, tok, *refs)

    projected, txt_parts = pl.pallas_call(
        body,
        out_shape=(
            jax.ShapeDtypeStruct((half, out_width), F32),
            jax.ShapeDtypeStruct((Y, Z, txt_q, HD), BF16),
        ),
        in_specs=[any_spec] * 3 + [vmem_spec] * 3 + [pl.BlockSpec(memory_space=pltpu.SMEM)],
        out_specs=(vmem_spec, any_spec),
        scratch_shapes=[
            vm((3, tok, width), BF16),
            vm(w_proj.shape, BF16),
            vm((txt_q, HD), BF16), vm((txt_k, HD), BF16), vm((txt_k, HD), BF16),
            vm((Z, 3, tok, HD), BF16),
            vm((X, Z, tok, HD), BF16),
            vm((Y, Z, 2, tok, HD), BF16),
            vm((X, block_n, HD), BF16), vm((X, strips, 1, HD), F32),
            vm((X, block_n, HD), BF16), vm((X, strips, 1, HD), F32),
            vm((txt_q, HD), BF16), vm((1, HD), F32),
            vm((X, txt_q, HD), BF16), vm((X, 1, HD), F32),
            vm((Z, tok, HD), BF16), vm((Z, tok, HD), BF16),
            vm((Y, Z, txt_q, HD), BF16),
            vm((half, out_width), F32), vm((cuts, half, wide), BF16), vm((cuts, half, wide), BF16),
            dma((5 + Y,)), dma((Z,)), dma((Z,)), dma(()), dma((X,)), dma(()), dma((Y,)), dma(()),
            dma((X,)), dma((X,)), dma((X,)), dma((X,)), dma((X,)), dma((X,)), dma((X,)), dma((X,)),
            dma(()), dma(()), dma(()), dma(()), dma((Y,)), dma(()), dma((cuts,)), dma((cuts,)),
        ],
        compiler_params=pltpu.CompilerParams(
            collective_id=0, has_side_effects=True, vmem_limit_bytes=56 * 1024 * 1024),
        name="joint_attention",
    )(qkv, txt, w_proj, frame_index, row_index, column_index, txt_len)

    img_out = (
        residual.astype(F32) + gate[None, None, :] * (projected[None] + proj_bias[None, None, :])
    ).astype(BF16)
    txt_out = txt_parts.transpose(0, 2, 1, 3).reshape(1, txt_total, width)
    return (img_out, txt_out)


def solution(mesh):
    shape = getattr(mesh, "solution_shape", (8, 4, 4))
    split = Mesh(mesh.devices.reshape(*shape, mesh.shape["tp"]), SEQ_TP)
    placed = (
        P(None, SEQ, None, "tp"),
        P(None, None, None, "tp"),
        P(None, SEQ),
        P(None, SEQ),
        P(None, SEQ),
        P(),
        P(None, SEQ_TP, None),
        P("tp", None),
        P(),
        P(),
    )
    return jax.shard_map(
        shards,
        mesh=split,
        in_specs=placed,
        out_specs=(P(None, SEQ_TP, None), P(None, None, "tp")),
        check_vma=False,
    )
```

```python
import math

import jax
import jax.numpy as jnp
from jax import lax
from jax.experimental import pallas as pl
from jax.experimental.pallas import tpu as pltpu
from jax.sharding import Mesh
from jax.sharding import PartitionSpec as P

HD = 128
AX_Z, AX_X, AX_Y, AX_C = "seq_0", "seq_1", "seq_2", "tp"
SEQ = (AX_Z, AX_X, AX_Y)
SEQ_TP = (AX_Z, AX_X, AX_Y, AX_C)
MESH = pl.DeviceIdType.MESH
F32 = jnp.float32
BF16 = jnp.bfloat16

rope_base = 256.0
neg_large = -1e30


def rope_in_kernel(frames, rows, columns, tok):
    part0 = HD // 8
    part1 = (HD - part0) // 2
    eye = lax.broadcasted_iota(jnp.int32, (tok, tok), 0) == lax.broadcasted_iota(jnp.int32, (tok, tok), 1)

    def column(ref):
        places = jnp.broadcast_to(ref[...].astype(F32), (tok, tok))
        return jnp.sum(jnp.where(eye, places, 0.0), axis=1, keepdims=True)

    lane = lax.broadcasted_iota(jnp.int32, (tok, HD), 1)
    in0 = lane < part0
    in1 = lane < part0 + part1
    start = jnp.where(in0, 0, jnp.where(in1, part0, part0 + part1))
    pair = ((lane - start) >> 1).astype(F32)
    width = jnp.where(in0, float(part0), float(part1))
    rate = jnp.exp(pair * (-2.0 * math.log(rope_base)) / width)
    place = jnp.where(in0, column(frames), jnp.where(in1, column(rows), column(columns)))
    angle = place * rate
    cosine, sine = jnp.cos(angle), jnp.sin(angle)
    even = (lane & 1) == 0
    return cosine, jnp.where(even, -sine, 0.0), jnp.where(even, 0.0, sine)


def kernel_body(
    Z, A, tok,
    qkv_hbm, txt_hbm, w_hbm, frames_hbm, rows_hbm, columns_hbm, txt_len, res_hbm, bias_hbm, gate_hbm,
    img_out, txt_out,
    qkv_v, w_v, frames, rows, columns, res_v, bias_v, gate_v, tq, tk, tv,
    send, qg, kvg, acc, peak_s, sum_s, ob, st, orecv, srecv, tob, tst, torecv, tsrecv,
    zs, ar, tbuf, pacc, part_own, part_send, part_recv,
    local_sem, zq_sem, zkv_sem, z_send, aq_sem, aq_send, bkv_sem, bkv_send,
    ao_sem, as_sem, ao_send, as_send, ato_sem, ats_sem, ato_send, ats_send,
    zo_sem, zo_send, t2_sem, t2_send, t3_sem, t3_send, c_sem, c_send,
):
    z, x, y, c = (lax.axis_index(axis) for axis in SEQ_TP)
    B = A
    a = x * (1 - c) + y * c
    b = y * (1 - c) + x * c
    txt_n = tq.shape[0]
    scale2 = math.log2(math.e) / math.sqrt(HD)

    def along_a(to):
        return {AX_X: to * (1 - c) + x * c, AX_Y: y * (1 - c) + to * c}

    def along_b(to):
        return {AX_X: x * (1 - c) + to * c, AX_Y: to * (1 - c) + y * c}

    def put(src, dst, ssem, rsem, device):
        pltpu.make_async_remote_copy(
            src_ref=src, dst_ref=dst, send_sem=ssem, recv_sem=rsem, device_id=device, device_id_type=MESH,
        ).start()

    def await_bytes(ref, sem):
        pltpu.make_async_copy(ref, ref, sem).wait()

    barrier = pltpu.get_barrier_semaphore()
    peers = 0
    for axis, size, me in ((AX_Z, Z, z), (AX_X, A, x), (AX_Y, A, y), (AX_C, 2, c)):
        for step in range(1, size):
            pl.semaphore_signal(barrier, inc=1, device_id={axis: lax.rem(me + step, size)}, device_id_type=MESH)
            peers += 1

    lane0 = pl.multiple_of(z * HD, HD)
    rows_b = pl.ds(pl.multiple_of(b * txt_n, txt_n), txt_n)
    rows_a = pl.ds(pl.multiple_of(a * txt_n, txt_n), txt_n)
    gets = [
        pltpu.make_async_copy(src, dst, local_sem.at[i])
        for i, (src, dst) in enumerate((
            (frames_hbm, frames), (rows_hbm, rows), (columns_hbm, columns),
            (qkv_hbm, qkv_v),
            (txt_hbm.at[0, rows_b, pl.ds(lane0, HD)], tq),
            (txt_hbm.at[1, rows_a, pl.ds(lane0, HD)], tk.at[0:txt_n]),
            (txt_hbm.at[2, rows_a, pl.ds(lane0, HD)], tv.at[0:txt_n]),
            (bias_hbm, bias_v), (gate_hbm, gate_v), (res_hbm, res_v), (w_hbm, w_v),
        ))
    ]
    for get in gets:
        get.start()

    for get in gets[:3]:
        get.wait()
    cosine, sine_even, sine_odd = rope_in_kernel(frames, rows, columns, tok)
    gets[3].wait()
    for h in range(Z):
        lanes = slice(h * HD, (h + 1) * HD)
        for kind in range(2):
            block = qkv_v[kind, :, lanes].astype(F32)
            turned = (
                block * cosine
                + pltpu.roll(block, HD - 1, 1) * sine_even
                + pltpu.roll(block, 1, 1) * sine_odd
            )
            send[h, kind] = turned.astype(BF16)
        send[h, 2] = qkv_v[2, :, lanes]
    qg[a, z] = send[z, 0]
    kvg[b, z] = send[z, 1:3]

    pl.semaphore_wait(barrier, peers)

    far_first = sorted(range(1, Z), key=lambda step: -min(step, Z - step))
    near_first = sorted(range(1, Z), key=lambda step: min(step, Z - step))
    for step in far_first:
        to = lax.rem(z + step, Z)
        put(send.at[to, 0], qg.at[a, z], z_send, zq_sem.at[z], {AX_Z: to})
    for step in far_first:
        to = lax.rem(z + step, Z)
        put(send.at[to, 1:3], kvg.at[b, z], z_send, zkv_sem.at[z], {AX_Z: to})

    hops = sorted(range(1, A), key=lambda hop: -min(hop, A - hop))
    for step in [0] + near_first:
        source = lax.rem(z + step, Z)
        if step:
            with jax.named_scope(f"wait_zq{step}"):
                await_bytes(qg.at[a, source], zq_sem.at[source])
        for hop in hops:
            put(qg.at[a, source], qg.at[a, source], aq_send, aq_sem.at[a], along_a(lax.rem(a + hop, A)))
    for step in [0] + near_first:
        source = lax.rem(z + step, Z)
        if step:
            with jax.named_scope(f"wait_zkv{step}"):
                await_bytes(kvg.at[b, source], zkv_sem.at[source])
        for hop in hops:
            put(kvg.at[b, source], kvg.at[b, source], bkv_send, bkv_sem.at[b], along_b(lax.rem(b + hop, B)))

    block_n = Z * tok
    strips = block_n // HD
    pad = tk.shape[0] - txt_n
    if pad:
        tk[txt_n:] = jnp.zeros((pad, HD), BF16)
        tv[txt_n:] = jnp.zeros((pad, HD), BF16)
    for get in gets[4:7]:
        get.wait()
    length = txt_len[0]
    live = lax.broadcasted_iota(jnp.int32, (1, tk.shape[0]), 1) < jnp.minimum(length - a * txt_n, txt_n)

    def scores_of(queries, keys):
        return lax.dot_general(queries, keys, (((1,), (1,)), ((), ())), preferred_element_type=F32)

    def to_row(col):
        n = col.shape[0]
        eye = lax.broadcasted_iota(jnp.int32, (n, HD), 0) == lax.broadcasted_iota(jnp.int32, (n, HD), 1)
        return jnp.sum(jnp.where(eye, col, 0.0), axis=0, keepdims=True)

    def to_col(row, n):
        eye = lax.broadcasted_iota(jnp.int32, (n, HD), 0) == lax.broadcasted_iota(jnp.int32, (n, HD), 1)
        return jnp.sum(jnp.where(eye, jnp.broadcast_to(row, (n, HD)), 0.0), axis=1, keepdims=True)

    def wide(col):
        return jnp.broadcast_to(col, (col.shape[0], HD))

    def absorb(slot, n, queries, keys, values, first):
        at = slice(slot * block_n, slot * block_n + n)
        scores = scores_of(queries, keys)
        parts = [scores[:, i:i + HD] for i in range(0, keys.shape[0], HD)]
        if first:
            txt_scores = jnp.where(live, scores_of(queries, tk[...]), neg_large)
            parts += [txt_scores[:, i:i + HD] for i in range(0, tk.shape[0], HD)]
        top = parts[0]
        for part in parts[1:]:
            top = jnp.maximum(top, part)
        peak = wide(jnp.max(top, axis=1, keepdims=True))
        if not first:
            old = peak_s[at]
            peak = jnp.maximum(peak, old)
            shrink = jnp.exp2((old - peak) * scale2)
        weights = [jnp.exp2((part - peak) * scale2) for part in parts]
        total = weights[0]
        for weight in weights[1:]:
            total = total + weight
        weights = [weight.astype(BF16) for weight in weights]
        image_parts = keys.shape[0] // HD
        blended = jnp.dot(
            jnp.concatenate(weights[:image_parts], axis=1), values, preferred_element_type=F32)
        if first:
            blended = blended + jnp.dot(
                jnp.concatenate(weights[image_parts:], axis=1), tv[...], preferred_element_type=F32)
        else:
            total = total + sum_s[at] * shrink
            blended = blended + acc[at] * shrink
        return at, peak, total, blended

    key_hops = [0] + sorted(range(1, B), key=lambda hop: min(hop, B - hop))
    query_hops = hops + [0]
    arrived = set()
    for key_hop in key_hops:
        first, last = key_hop == key_hops[0], key_hop == key_hops[-1]
        other = lax.rem(b + key_hop, B)
        if not first:
            with jax.named_scope(f"wait_kv{key_hop}"):
                await_bytes(kvg.at[other], bkv_sem.at[other])
        keys = kvg[other, :, 0].reshape(block_n, HD)
        values = kvg[other, :, 1].reshape(block_n, HD)
        for hop in [None] + ([0] + hops[::-1] if first else query_hops):
            if hop is None:
                slot, n, queries = A, txt_n, tq[...]
            else:
                slot, n, to = hop, block_n, lax.rem(a + hop, A)
                if first and hop:
                    with jax.named_scope(f"wait_q{hop}"):
                        await_bytes(qg.at[to], aq_sem.at[to])
                queries = qg[to].reshape(block_n, HD)
            at, peak, total, blended = absorb(slot, n, queries, keys, values, first)
            if not last:
                peak_s[at], sum_s[at], acc[at] = peak, total, blended
                continue
            weight_sum = jnp.sum(total, axis=1, keepdims=True)
            result = (blended / weight_sum).astype(BF16)
            log = peak * scale2 + jnp.log2(weight_sum)
            if hop is None:
                tob[...] = result
                tst[...] = to_row(log)
                for via in hops:
                    dev = along_a(lax.rem(a + via, A))
                    put(tob, torecv.at[a], ato_send.at[via], ato_sem.at[a], dev)
                    put(tst, tsrecv.at[a], ats_send.at[via], ats_sem.at[a], dev)
                continue
            ob[hop] = result
            for strip in range(strips):
                st[hop, strip] = to_row(log[strip * HD:(strip + 1) * HD])
            if hop:
                put(ob.at[hop], orecv.at[a], ao_send.at[hop], ao_sem.at[a], along_a(to))
                put(st.at[hop], srecv.at[a], as_send.at[hop], as_sem.at[a], along_a(to))

    def merge(parts, logs):
        top = logs[0]
        for log in logs[1:]:
            top = jnp.maximum(top, log)
        shares = [jnp.exp2(log - top) for log in logs]
        return sum(part * share for part, share in zip(parts, shares)) / sum(shares)

    parts, logs = [tob[...].astype(F32)], [to_col(tst[...], txt_n)]
    for hop in hops[::-1]:
        other = lax.rem(a + hop, A)
        await_bytes(torecv.at[other], ato_sem.at[other])
        await_bytes(tsrecv.at[other], ats_sem.at[other])
        parts.append(torecv[other].astype(F32))
        logs.append(to_col(tsrecv[other], txt_n))
    kept = lax.broadcasted_iota(jnp.int32, (txt_n, 1), 0) + b * txt_n < length
    tbuf[b, z] = jnp.where(kept, merge(parts, logs), 0.0).astype(BF16)
    for step in far_first:
        put(tbuf.at[b, z], tbuf.at[b, z], t2_send, t2_sem.at[z], {AX_Z: lax.rem(z + step, Z)})

    for hop in hops:
        other = lax.rem(a + hop, A)
        await_bytes(orecv.at[other], ao_sem.at[other])
        await_bytes(srecv.at[other], as_sem.at[other])
    per = HD // tok
    for strip in range(strips):
        at = slice(strip * HD, (strip + 1) * HD)
        parts, logs = [ob[0, at].astype(F32)], [to_col(st[0, strip], HD)]
        for hop in hops:
            other = lax.rem(a + hop, A)
            parts.append(orecv[other, at].astype(F32))
            logs.append(to_col(srecv[other, strip], HD))
        zs[strip * per:(strip + 1) * per] = merge(parts, logs).astype(BF16).reshape(per, tok, HD)
    for step in far_first:
        to = lax.rem(z + step, Z)
        put(zs.at[to], ar.at[z], zo_send, zo_sem.at[z], {AX_Z: to})

    gets[-1].wait()
    half = tok // 2
    cuts = part_send.shape[0]
    width = part_send.shape[2]
    ar[z] = zs[z]
    for step in [0] + near_first:
        source = lax.rem(z + step, Z)
        if step:
            with jax.named_scope(f"wait_txt{step}"):
                await_bytes(tbuf.at[b, source], t2_sem.at[source])
        for hop in hops:
            put(tbuf.at[b, source], tbuf.at[b, source], t3_send, t3_sem.at[b], along_b(lax.rem(b + hop, B)))
        if step:
            with jax.named_scope(f"wait_home{step}"):
                await_bytes(ar.at[source], zo_sem.at[source])
        depth = pl.ds(pl.multiple_of(source * HD, HD), HD)
        for cut in range(cuts):
            lanes = slice(cut * width, (cut + 1) * width)
            product = jnp.dot(ar[source], w_v[depth, lanes], preferred_element_type=F32)
            if step:
                product = product + pacc[:, lanes]
            if step != near_first[-1]:
                pacc[:, lanes] = product
                continue
            upper, lower = product[:half], product[half:]
            part_own[:, lanes] = jnp.where(c == 0, upper, lower)
            part_send[cut] = jnp.where(c == 0, lower, upper).astype(BF16)
            put(part_send.at[cut], part_recv.at[cut], c_send.at[cut], c_sem.at[cut], {AX_C: 1 - c})

    for get in gets[7:10]:
        get.wait()
    for cut in range(cuts):
        lanes = slice(cut * width, (cut + 1) * width)
        await_bytes(part_recv.at[cut], c_sem.at[cut])
        projected = part_own[:, lanes] + part_recv[cut].astype(F32)
        img_out[:, lanes] = (
            res_v[:, lanes].astype(F32) + gate_v[:, lanes] * (projected + bias_v[:, lanes])
        ).astype(BF16)

    for hop in [0] + hops[::-1]:
        other = lax.rem(b + hop, B)
        if hop:
            await_bytes(tbuf.at[other], t3_sem.at[other])
        at = pl.ds(pl.multiple_of(other * txt_n, txt_n), txt_n)
        for h in range(Z):
            txt_out[at, h * HD:(h + 1) * HD] = tbuf[other, h]

    await_bytes(send.at[0:Z - 1], z_send)
    await_bytes(kvg.at[0:B - 1], bkv_send)
    await_bytes(qg.at[0:A - 1], aq_send)
    for hop in range(1, A):
        await_bytes(tob, ato_send.at[hop])
        await_bytes(tst, ats_send.at[hop])
        await_bytes(ob.at[hop], ao_send.at[hop])
        await_bytes(st.at[hop], as_send.at[hop])
    await_bytes(zs.at[0:Z - 1], zo_send)
    await_bytes(tbuf.at[0, 0:Z - 1], t2_send)
    await_bytes(tbuf.at[0:B - 1], t3_send)
    for cut in range(cuts):
        await_bytes(part_send.at[cut], c_send.at[cut])


def shards(
    img_qkv, txt_qkv, frame_index, row_index, column_index, txt_len, residual, w_proj, proj_bias, gate,
):
    Z, A, B = (lax.axis_size(axis) for axis in SEQ)
    tok = img_qkv.shape[1]
    width = img_qkv.shape[3]
    txt_total = txt_qkv.shape[1]
    out_width = w_proj.shape[1]
    txt_n = txt_total // A
    txt_pad = -(-txt_n // HD) * HD
    cuts = 6
    wide = out_width // cuts
    half = tok // 2
    block_n = Z * tok
    strips = block_n // HD
    rows_n = A * block_n + txt_n

    qkv = jnp.transpose(img_qkv[0], (1, 0, 2))
    txt = jnp.transpose(txt_qkv[0], (1, 0, 2))
    dma = pltpu.SemaphoreType.DMA
    vm = pltpu.VMEM
    hbm_spec = pl.BlockSpec(memory_space=pltpu.HBM)
    vmem_spec = pl.BlockSpec(memory_space=pltpu.VMEM)

    def body(*refs):
        kernel_body(Z, A, tok, *refs)

    img_v, txt_v = pl.pallas_call(
        body,
        out_shape=(pltpu.VMEM((half, out_width), BF16), pltpu.VMEM((txt_total, width), BF16)),
        in_specs=[hbm_spec] * 6 + [pl.BlockSpec(memory_space=pltpu.SMEM)] + [hbm_spec] * 3,
        out_specs=(vmem_spec, vmem_spec),
        scratch_shapes=[
            vm((3, tok, width), BF16),
            vm(w_proj.shape, BF16),
            vm((1, tok), jnp.int32), vm((1, tok), jnp.int32), vm((1, tok), jnp.int32),
            vm((half, out_width), BF16), vm((1, out_width), F32), vm((1, out_width), F32),
            vm((txt_n, HD), BF16), vm((txt_pad, HD), BF16), vm((txt_pad, HD), BF16),
            vm((Z, 3, tok, HD), BF16),
            vm((A, Z, tok, HD), BF16),
            vm((B, Z, 2, tok, HD), BF16),
            vm((rows_n, HD), F32), vm((rows_n, HD), F32), vm((rows_n, HD), F32),
            vm((A, block_n, HD), BF16), vm((A, strips, 1, HD), F32),
            vm((A, block_n, HD), BF16), vm((A, strips, 1, HD), F32),
            vm((txt_n, HD), BF16), vm((1, HD), F32),
            vm((A, txt_n, HD), BF16), vm((A, 1, HD), F32),
            vm((Z, tok, HD), BF16), vm((Z, tok, HD), BF16),
            vm((B, Z, txt_n, HD), BF16),
            vm((tok, out_width), F32),
            vm((half, out_width), F32), vm((cuts, half, wide), BF16), vm((cuts, half, wide), BF16),
            dma((11,)), dma((Z,)), dma((Z,)), dma(()), dma((A,)), dma(()), dma((B,)), dma(()),
            dma((A,)), dma((A,)), dma((A,)), dma((A,)), dma((A,)), dma((A,)), dma((A,)), dma((A,)),
            dma((Z,)), dma(()), dma((Z,)), dma(()), dma((B,)), dma(()), dma((cuts,)), dma((cuts,)),
        ],
        compiler_params=pltpu.CompilerParams(
            collective_id=0, has_side_effects=True, vmem_limit_bytes=24 * 1024 * 1024),
        name="joint_attention",
    )(*(
        operand if operand is txt_len else pltpu.with_memory_space_constraint(operand, pltpu.HBM)
        for operand in (
            qkv, txt, w_proj, frame_index, row_index, column_index, txt_len, residual[0],
            proj_bias.reshape(1, -1), gate.reshape(1, -1),
        )
    ))

    def write_out(img_ref, txt_ref, img_hbm, txt_hbm, sems):
        outs = [
            pltpu.make_async_copy(img_ref, img_hbm, sems.at[0]),
            pltpu.make_async_copy(txt_ref, txt_hbm, sems.at[1]),
        ]
        for out in outs:
            out.start()
        for out in outs:
            out.wait()

    img_out, txt_out = pl.pallas_call(
        write_out,
        out_shape=(
            jax.ShapeDtypeStruct((half, out_width), BF16),
            jax.ShapeDtypeStruct((txt_total, width), BF16),
        ),
        in_specs=[vmem_spec] * 2,
        out_specs=(hbm_spec, hbm_spec),
        scratch_shapes=[dma((2,))],
        compiler_params=pltpu.CompilerParams(vmem_limit_bytes=1024 * 1024),
        name="write_out",
    )(img_v, txt_v)
    return (img_out[None], txt_out[None])


def solution(mesh):
    shape = getattr(mesh, "solution_shape", (8, 4, 4))
    split = Mesh(mesh.devices.reshape(*shape, mesh.shape["tp"]), SEQ_TP)
    placed = (
        P(None, SEQ, None, "tp"),
        P(None, None, None, "tp"),
        P(None, SEQ),
        P(None, SEQ),
        P(None, SEQ),
        P(),
        P(None, SEQ_TP, None),
        P("tp", None),
        P(),
        P(),
    )
    return jax.shard_map(
        shards,
        mesh=split,
        in_specs=placed,
        out_specs=(P(None, SEQ_TP, None), P(None, None, "tp")),
        check_vma=False,
    )
```

```python
import math

import jax
import jax.numpy as jnp
from jax import lax
from jax.experimental import pallas as pl
from jax.experimental.pallas import tpu as pltpu
from jax.sharding import Mesh
from jax.sharding import PartitionSpec as P

HD = 128
AX_Z, AX_X, AX_Y, AX_C = "seq_0", "seq_1", "seq_2", "tp"
SEQ = (AX_Z, AX_X, AX_Y)
SEQ_TP = (AX_Z, AX_X, AX_Y, AX_C)
MESH = pl.DeviceIdType.MESH
F32 = jnp.float32
BF16 = jnp.bfloat16

rope_base = 256.0
neg_large = -1e30


def rope_in_kernel(frames, rows, columns, tok):
    part0 = HD // 8
    part1 = (HD - part0) // 2
    eye = lax.broadcasted_iota(jnp.int32, (tok, tok), 0) == lax.broadcasted_iota(jnp.int32, (tok, tok), 1)

    def column(ref):
        places = jnp.broadcast_to(ref[...].astype(F32), (tok, tok))
        return jnp.sum(jnp.where(eye, places, 0.0), axis=1, keepdims=True)

    lane = lax.broadcasted_iota(jnp.int32, (tok, HD), 1)
    in0 = lane < part0
    in1 = lane < part0 + part1
    start = jnp.where(in0, 0, jnp.where(in1, part0, part0 + part1))
    pair = ((lane - start) >> 1).astype(F32)
    width = jnp.where(in0, float(part0), float(part1))
    rate = jnp.exp(pair * (-2.0 * math.log(rope_base)) / width)
    place = jnp.where(in0, column(frames), jnp.where(in1, column(rows), column(columns)))
    angle = place * rate
    cosine, sine = jnp.cos(angle), jnp.sin(angle)
    even = (lane & 1) == 0
    return cosine, jnp.where(even, -sine, 0.0), jnp.where(even, 0.0, sine)


def kernel_body(
    Z, A, tok,
    qkv_hbm, txt_hbm, w_hbm, frames_hbm, rows_hbm, columns_hbm, txt_len, res_hbm, bias_hbm, gate_hbm,
    img_out, txt_out,
    qkv_v, w_v, frames, rows, columns, res_v, bias_v, gate_v, tq, tk, tv,
    send, qg, kvg, acc, peak_s, sum_s, ob, st, orecv, srecv, tob, tst, torecv, tsrecv,
    zs, ar, tbuf, pacc, part_own, part_send, part_recv,
    local_sem, zq_sem, zkv_sem, aq_sem, bkv_sem, ao_sem, as_sem, ato_sem, ats_sem,
    zo_sem, t2_sem, t3_sem, c_sem, send_sem, log_send,
):
    z, x, y, c = (lax.axis_index(axis) for axis in SEQ_TP)
    B = A
    a = x * (1 - c) + y * c
    b = y * (1 - c) + x * c
    txt_n = tq.shape[0]
    scale2 = math.log2(math.e) / math.sqrt(HD)

    def along_a(to):
        return {AX_X: to * (1 - c) + x * c, AX_Y: y * (1 - c) + to * c}

    def along_b(to):
        return {AX_X: x * (1 - c) + to * c, AX_Y: to * (1 - c) + y * c}

    def put(src, dst, ssem, rsem, device):
        pltpu.make_async_remote_copy(
            src_ref=src, dst_ref=dst, send_sem=ssem, recv_sem=rsem, device_id=device, device_id_type=MESH,
        ).start()

    def await_bytes(ref, sem):
        pltpu.make_async_copy(ref, ref, sem).wait()

    barrier = pltpu.get_barrier_semaphore()
    peers = 0
    for axis, size, me in ((AX_Z, Z, z), (AX_X, A, x), (AX_Y, A, y), (AX_C, 2, c)):
        for step in range(1, size):
            pl.semaphore_signal(barrier, inc=1, device_id={axis: lax.rem(me + step, size)}, device_id_type=MESH)
            peers += 1

    lane0 = pl.multiple_of(z * HD, HD)
    rows_b = pl.ds(pl.multiple_of(b * txt_n, txt_n), txt_n)
    rows_a = pl.ds(pl.multiple_of(a * txt_n, txt_n), txt_n)
    gets = [
        pltpu.make_async_copy(src, dst, local_sem.at[i])
        for i, (src, dst) in enumerate((
            (frames_hbm, frames), (rows_hbm, rows), (columns_hbm, columns),
            (qkv_hbm, qkv_v),
            (txt_hbm.at[0, rows_b, pl.ds(lane0, HD)], tq),
            (txt_hbm.at[1, rows_a, pl.ds(lane0, HD)], tk.at[0:txt_n]),
            (txt_hbm.at[2, rows_a, pl.ds(lane0, HD)], tv.at[0:txt_n]),
            (bias_hbm, bias_v), (gate_hbm, gate_v), (res_hbm, res_v), (w_hbm, w_v),
        ))
    ]
    for get in gets:
        get.start()

    for get in gets[:3]:
        get.wait()
    cosine, sine_even, sine_odd = rope_in_kernel(frames, rows, columns, tok)
    gets[3].wait()
    for h in range(Z):
        lanes = slice(h * HD, (h + 1) * HD)
        for kind in range(2):
            block = qkv_v[kind, :, lanes].astype(F32)
            turned = (
                block * cosine
                + pltpu.roll(block, HD - 1, 1) * sine_even
                + pltpu.roll(block, 1, 1) * sine_odd
            )
            send[h, kind] = turned.astype(BF16)
        send[h, 2] = qkv_v[2, :, lanes]
    qg[a, z] = send[z, 0]
    kvg[b, z] = send[z, 1:3]

    pl.semaphore_wait(barrier, peers)

    def apart(step):
        return min(step, Z - step) - 1

    pairs = [[0]] + [sorted({d, Z - d}) for d in range(1, Z // 2 + 1)]
    far_first = sorted(range(1, Z), key=lambda step: -min(step, Z - step))
    near_first = sorted(range(1, Z), key=lambda step: min(step, Z - step))
    for step in far_first:
        to = lax.rem(z + step, Z)
        put(send.at[to, 0], qg.at[a, z], send_sem, zq_sem.at[apart(step)], {AX_Z: to})
    for step in far_first:
        to = lax.rem(z + step, Z)
        put(send.at[to, 1:3], kvg.at[b, z], send_sem, zkv_sem.at[apart(step)], {AX_Z: to})

    hops = sorted(range(1, A), key=lambda hop: -min(hop, A - hop))
    for pair in pairs:
        if pair[0]:
            with jax.named_scope(f"wait_zq{pair[0]}"):
                await_bytes(qg.at[a, 0:len(pair)], zq_sem.at[apart(pair[0])])
        for step in pair:
            source = lax.rem(z + step, Z)
            for hop in hops:
                put(qg.at[a, source], qg.at[a, source], send_sem, aq_sem, along_a(lax.rem(a + hop, A)))
    for pair in pairs:
        if pair[0]:
            with jax.named_scope(f"wait_zkv{pair[0]}"):
                await_bytes(kvg.at[b, 0:len(pair)], zkv_sem.at[apart(pair[0])])
        for step in pair:
            source = lax.rem(z + step, Z)
            for hop in hops:
                put(kvg.at[b, source], kvg.at[b, source], send_sem, bkv_sem.at[hop], along_b(lax.rem(b + hop, B)))

    block_n = Z * tok
    strips = block_n // HD
    pad = tk.shape[0] - txt_n
    if pad:
        tk[txt_n:] = jnp.zeros((pad, HD), BF16)
        tv[txt_n:] = jnp.zeros((pad, HD), BF16)
    for get in gets[4:7]:
        get.wait()
    length = txt_len[0]
    live = lax.broadcasted_iota(jnp.int32, (1, tk.shape[0]), 1) < jnp.minimum(length - a * txt_n, txt_n)

    def scores_of(queries, keys):
        return lax.dot_general(queries, keys, (((1,), (1,)), ((), ())), preferred_element_type=F32)

    def to_row(col):
        n = col.shape[0]
        eye = lax.broadcasted_iota(jnp.int32, (n, HD), 0) == lax.broadcasted_iota(jnp.int32, (n, HD), 1)
        return jnp.sum(jnp.where(eye, col, 0.0), axis=0, keepdims=True)

    def to_col(row, n):
        eye = lax.broadcasted_iota(jnp.int32, (n, HD), 0) == lax.broadcasted_iota(jnp.int32, (n, HD), 1)
        return jnp.sum(jnp.where(eye, jnp.broadcast_to(row, (n, HD)), 0.0), axis=1, keepdims=True)

    def wide(col):
        return jnp.broadcast_to(col, (col.shape[0], HD))

    def rows_of(hop, to_hop=None):
        to_hop = hop if to_hop is None else to_hop
        return slice(txt_n + hop * block_n, txt_n + (to_hop + 1) * block_n)

    txt_rows = slice(0, txt_n)

    def image_queries(*hop_list):
        return [qg[lax.rem(a + hop, A)].reshape(block_n, HD) for hop in hop_list]

    def absorb(at, queries, keys, values, first):
        queries = jnp.concatenate(queries, axis=0) if len(queries) > 1 else queries[0]
        scores = scores_of(queries, keys)
        parts = [scores[:, i:i + HD] for i in range(0, keys.shape[0], HD)]
        if first:
            txt_scores = jnp.where(live, scores_of(queries, tk[...]), neg_large)
            parts += [txt_scores[:, i:i + HD] for i in range(0, tk.shape[0], HD)]
        top = parts[0]
        for part in parts[1:]:
            top = jnp.maximum(top, part)
        peak = wide(jnp.max(top, axis=1, keepdims=True))
        if not first:
            old = peak_s[at]
            peak = jnp.maximum(peak, old)
            shrink = jnp.exp2((old - peak) * scale2)
        weights = [jnp.exp2((part - peak) * scale2) for part in parts]
        total = weights[0]
        for weight in weights[1:]:
            total = total + weight
        weights = [weight.astype(BF16) for weight in weights]
        image_parts = keys.shape[0] // HD
        blended = jnp.dot(
            jnp.concatenate(weights[:image_parts], axis=1), values, preferred_element_type=F32)
        if first:
            blended = blended + jnp.dot(
                jnp.concatenate(weights[image_parts:], axis=1), tv[...], preferred_element_type=F32)
        else:
            total = total + sum_s[at] * shrink
            blended = blended + acc[at] * shrink
        return peak, total, blended

    def finish(state):
        peak, total, blended = state
        weight_sum = jnp.sum(total, axis=1, keepdims=True)
        return (blended / weight_sum).astype(BF16), peak * scale2 + jnp.log2(weight_sum)

    def finish_image(lo, hi, keys, values):
        result, log = finish(
            absorb(rows_of(lo, hi), image_queries(*range(lo, hi + 1)), keys, values, False))
        for hop in range(lo, hi + 1):
            base = (hop - lo) * block_n
            ob[hop] = result[base:base + block_n]
            for strip in range(strips):
                st[hop, strip] = to_row(log[base + strip * HD:base + (strip + 1) * HD])

    def keep(at, state):
        peak_s[at], sum_s[at], acc[at] = state

    key_hops = [0] + sorted(range(1, B), key=lambda hop: min(hop, B - hop))
    all_rows = slice(0, txt_n + A * block_n)
    for key_hop in key_hops:
        first, last = key_hop == key_hops[0], key_hop == key_hops[-1]
        other = lax.rem(b + key_hop, B)
        if not first:
            with jax.named_scope(f"wait_kv{key_hop}"):
                await_bytes(kvg.at[other], bkv_sem.at[B - key_hop])
        keys = kvg[other, :, 0].reshape(block_n, HD)
        values = kvg[other, :, 1].reshape(block_n, HD)
        if first:
            near_rows, far_rows = slice(0, txt_n + block_n), rows_of(1, A - 1)
            keep(near_rows, absorb(near_rows, [tq[...]] + image_queries(0), keys, values, True))
            with jax.named_scope("wait_q"):
                await_bytes(qg.at[0:A - 1], aq_sem)
            keep(far_rows, absorb(far_rows, image_queries(*range(1, A)), keys, values, True))
        elif not last:
            keep(all_rows, absorb(
                all_rows, [tq[...]] + image_queries(*range(A)), keys, values, False))
    result, log = finish(absorb(txt_rows, [tq[...]], keys, values, False))
    tob[...], tst[...] = result, to_row(log)
    for hop in hops:
        to = along_a(lax.rem(a + hop, A))
        put(tob, torecv.at[a], send_sem, ato_sem, to)
        put(tst, tsrecv.at[a], log_send.at[0], ats_sem, to)
    finish_image(1, A - 1, keys, values)
    for hop in hops:
        to = along_a(lax.rem(a + hop, A))
        put(ob.at[hop], orecv.at[a], send_sem, ao_sem, to)
        put(st.at[hop], srecv.at[a], log_send.at[1], as_sem, to)
    finish_image(0, 0, keys, values)

    others_up = [i + jnp.where(z <= i, 1, 0) for i in range(Z - 1)]

    def far(to):
        gap = lax.rem(to - z + Z, Z)
        return jnp.minimum(gap, Z - gap) - 1

    def merge(parts, logs):
        top = logs[0]
        for log in logs[1:]:
            top = jnp.maximum(top, log)
        shares = [jnp.exp2(log - top) for log in logs]
        return sum(part * share for part, share in zip(parts, shares)) / sum(shares)

    await_bytes(torecv.at[0:A - 1], ato_sem)
    await_bytes(tsrecv.at[0:A - 1], ats_sem)
    parts, logs = [tob[...].astype(F32)], [to_col(tst[...], txt_n)]
    for hop in hops[::-1]:
        other = lax.rem(a + hop, A)
        parts.append(torecv[other].astype(F32))
        logs.append(to_col(tsrecv[other], txt_n))
    kept = lax.broadcasted_iota(jnp.int32, (txt_n, 1), 0) + b * txt_n < length
    tbuf[b, z] = jnp.where(kept, merge(parts, logs), 0.0).astype(BF16)
    for to in others_up:
        put(tbuf.at[b, z], tbuf.at[b, z], send_sem, t2_sem.at[far(to)], {AX_Z: to})

    await_bytes(orecv.at[0:A - 1], ao_sem)
    await_bytes(srecv.at[0:A - 1], as_sem)
    per = HD // tok
    for strip in range(strips):
        at = slice(strip * HD, (strip + 1) * HD)
        parts, logs = [ob[0, at].astype(F32)], [to_col(st[0, strip], HD)]
        for hop in hops:
            other = lax.rem(a + hop, A)
            parts.append(orecv[other, at].astype(F32))
            logs.append(to_col(srecv[other, strip], HD))
        zs[strip * per:(strip + 1) * per] = merge(parts, logs).astype(BF16).reshape(per, tok, HD)
    for to in others_up:
        put(zs.at[to], ar.at[z], send_sem, zo_sem.at[far(to)], {AX_Z: to})

    gets[-1].wait()
    half = tok // 2
    cuts = part_send.shape[0]
    width = part_send.shape[2]
    ar[z] = zs[z]
    def text_on(pair):
        if pair[0]:
            with jax.named_scope(f"wait_txt{pair[0]}"):
                await_bytes(tbuf.at[b, 0:len(pair)], t2_sem.at[apart(pair[0])])
        for step in pair:
            source = lax.rem(z + step, Z)
            for hop in hops:
                put(tbuf.at[b, source], tbuf.at[b, source], send_sem, t3_sem, along_b(lax.rem(b + hop, B)))

    def project(step):
        source = lax.rem(z + step, Z)
        depth = pl.ds(pl.multiple_of(source * HD, HD), HD)
        for cut in range(cuts):
            lanes = slice(cut * width, (cut + 1) * width)
            product = jnp.dot(ar[source], w_v[depth, lanes], preferred_element_type=F32)
            if step:
                product = product + pacc[:, lanes]
            if step != pairs[-1][-1]:
                pacc[:, lanes] = product
                continue
            upper, lower = product[:half], product[half:]
            part_own[:, lanes] = jnp.where(c == 0, upper, lower)
            part_send[cut] = jnp.where(c == 0, lower, upper).astype(BF16)
            put(part_send.at[cut], part_recv.at[cut], send_sem, c_sem.at[cut // 2], {AX_C: 1 - c})

    def home(pair):
        if pair[0]:
            with jax.named_scope(f"wait_home{pair[0]}"):
                await_bytes(ar.at[0:len(pair)], zo_sem.at[apart(pair[0])])
        for step in pair:
            project(step)

    text_on(pairs[0])
    home(pairs[0])
    text_on(pairs[1])
    for pair, behind in zip(pairs[2:], pairs[1:]):
        text_on(pair)
        home(behind)
    home(pairs[-1])

    for get in gets[7:10]:
        get.wait()
    for cut in range(cuts):
        lanes = slice(cut * width, (cut + 1) * width)
        if cut % 2 == 0:
            await_bytes(part_recv.at[cut:cut + 2], c_sem.at[cut // 2])
        projected = part_own[:, lanes] + part_recv[cut].astype(F32)
        img_out[:, lanes] = (
            res_v[:, lanes].astype(F32) + gate_v[:, lanes] * (projected + bias_v[:, lanes])
        ).astype(BF16)

    await_bytes(tbuf.at[0:B - 1], t3_sem)
    for part in range(B):
        for h in range(Z):
            txt_out[part * txt_n:(part + 1) * txt_n, h * HD:(h + 1) * HD] = tbuf[part, h]

    sent = (
        (Z - 1) * math.prod(send.shape[1:]) + (A - 1) * math.prod(qg.shape[1:]) + (B - 1) * math.prod(kvg.shape[1:]) + (A - 1) * (math.prod(tob.shape) + math.prod(ob.shape[1:]))
        + (Z - 1) * (math.prod(tbuf.shape[2:]) + math.prod(zs.shape[1:])) + (B - 1) * math.prod(tbuf.shape[1:]) + math.prod(part_send.shape)
    )
    assert sent % w_v.shape[1] == 0
    await_bytes(w_v.at[0:sent // w_v.shape[1]], send_sem)
    await_bytes(tsrecv.at[0:A - 1], log_send.at[0])
    await_bytes(st.at[0:A - 1], log_send.at[1])


def shards(
    img_qkv, txt_qkv, frame_index, row_index, column_index, txt_len, residual, w_proj, proj_bias, gate,
):
    Z, A, B = (lax.axis_size(axis) for axis in SEQ)
    tok = img_qkv.shape[1]
    width = img_qkv.shape[3]
    txt_total = txt_qkv.shape[1]
    out_width = w_proj.shape[1]
    txt_n = txt_total // A
    txt_pad = -(-txt_n // HD) * HD
    cuts = 6
    wide = out_width // cuts
    half = tok // 2
    block_n = Z * tok
    strips = block_n // HD
    rows_n = A * block_n + txt_n

    qkv = jnp.transpose(img_qkv[0], (1, 0, 2))
    txt = jnp.transpose(txt_qkv[0], (1, 0, 2))
    dma = pltpu.SemaphoreType.DMA
    vm = pltpu.VMEM
    hbm_spec = pl.BlockSpec(memory_space=pltpu.HBM)
    vmem_spec = pl.BlockSpec(memory_space=pltpu.VMEM)

    def body(*refs):
        kernel_body(Z, A, tok, *refs)

    img_v, txt_v = pl.pallas_call(
        body,
        out_shape=(pltpu.VMEM((half, out_width), BF16), pltpu.VMEM((txt_total, width), BF16)),
        in_specs=[hbm_spec] * 6 + [pl.BlockSpec(memory_space=pltpu.SMEM)] + [hbm_spec] * 3,
        out_specs=(vmem_spec, vmem_spec),
        scratch_shapes=[
            vm((3, tok, width), BF16),
            vm(w_proj.shape, BF16),
            vm((1, tok), jnp.int32), vm((1, tok), jnp.int32), vm((1, tok), jnp.int32),
            vm((half, out_width), BF16), vm((1, out_width), F32), vm((1, out_width), F32),
            vm((txt_n, HD), BF16), vm((txt_pad, HD), BF16), vm((txt_pad, HD), BF16),
            vm((Z, 3, tok, HD), BF16),
            vm((A, Z, tok, HD), BF16),
            vm((B, Z, 2, tok, HD), BF16),
            vm((rows_n, HD), F32), vm((rows_n, HD), F32), vm((rows_n, HD), F32),
            vm((A, block_n, HD), BF16), vm((A, strips, 1, HD), F32),
            vm((A, block_n, HD), BF16), vm((A, strips, 1, HD), F32),
            vm((txt_n, HD), BF16), vm((1, HD), F32),
            vm((A, txt_n, HD), BF16), vm((A, 1, HD), F32),
            vm((Z, tok, HD), BF16), vm((Z, tok, HD), BF16),
            vm((B, Z, txt_n, HD), BF16),
            vm((tok, out_width), F32),
            vm((half, out_width), F32), vm((cuts, half, wide), BF16), vm((cuts, half, wide), BF16),
            dma((11,)), dma((Z // 2,)), dma((Z // 2,)), dma(()), dma((B,)), dma(()), dma(()), dma(()), dma(()),
            dma((Z // 2,)), dma((Z // 2,)), dma(()), dma((cuts // 2,)), dma(()), dma((2,)),
        ],
        compiler_params=pltpu.CompilerParams(
            collective_id=0, has_side_effects=True, vmem_limit_bytes=24 * 1024 * 1024),
        name="joint_attention",
    )(*(
        operand if operand is txt_len else pltpu.with_memory_space_constraint(operand, pltpu.HBM)
        for operand in (
            qkv, txt, w_proj, frame_index, row_index, column_index, txt_len, residual[0],
            proj_bias.reshape(1, -1), gate.reshape(1, -1),
        )
    ))

    def write_out(img_ref, txt_ref, img_hbm, txt_hbm, sems):
        outs = [
            pltpu.make_async_copy(img_ref, img_hbm, sems.at[0]),
            pltpu.make_async_copy(txt_ref, txt_hbm, sems.at[1]),
        ]
        for out in outs:
            out.start()
        for out in outs:
            out.wait()

    img_out, txt_out = pl.pallas_call(
        write_out,
        out_shape=(
            jax.ShapeDtypeStruct((half, out_width), BF16),
            jax.ShapeDtypeStruct((txt_total, width), BF16),
        ),
        in_specs=[vmem_spec] * 2,
        out_specs=(hbm_spec, hbm_spec),
        scratch_shapes=[dma((2,))],
        compiler_params=pltpu.CompilerParams(vmem_limit_bytes=1024 * 1024),
        name="write_out",
    )(img_v, txt_v)
    return (img_out[None], txt_out[None])


def solution(mesh):
    shape = getattr(mesh, "solution_shape", (8, 4, 4))
    split = Mesh(mesh.devices.reshape(*shape, mesh.shape["tp"]), SEQ_TP)
    placed = (
        P(None, SEQ, None, "tp"),
        P(None, None, None, "tp"),
        P(None, SEQ),
        P(None, SEQ),
        P(None, SEQ),
        P(),
        P(None, SEQ_TP, None),
        P("tp", None),
        P(),
        P(),
    )
    return jax.shard_map(
        shards,
        mesh=split,
        in_specs=placed,
        out_specs=(P(None, SEQ_TP, None), P(None, None, "tp")),
        check_vma=False,
    )
```
